32 devices in a mesh: grp: 2 (over x), src: 8 (over z, y), tgt: 2 (over core).
Axes of the slice: x: 2, y: 2, z: 4, core: 2. Of those that a mesh axis runs over, the one named last changes fastest.
Arguments:
- densities: bfloat16 [512, 32768], P('grp', ('src', 'tgt')), parts along dimension 0, may hold values from -6 to 6
- compress: bfloat16 [65536, 2, 256], P(('grp', 'src', 'tgt')), parts along dimension 0, may hold values from -0.0625 to 0.0625
- level_a: bfloat16 [6, 2048, 2, 256], P('grp', 'src', None, 'tgt'), parts along dimension 0, may hold values from -0.1875 to 0.1875
- level_b: bfloat16 [6, 2048, 2, 256], P('grp', 'src', None, 'tgt'), parts along dimension 0, may hold values from -0.1875 to 0.1875
- expand: bfloat16 [4096, 2, 4096], P(('grp', 'src'), None, 'tgt'), parts along dimension 0, may hold values from -0.25 to 0.25
- near_tiles: bfloat16 [2048, 128, 2, 128], P(('grp', 'src', 'tgt')), parts along dimension 0, may hold values from -0.375 to 0.375
- tile_pairs: int32 [2048, 2], P(('grp', 'src', 'tgt')), parts along dimension 0, may hold values from 0 to 15
- tile_count: int32 [32], P(('grp', 'src', 'tgt')), parts along dimension 0, may hold values from 1 to 63, as said below
- cluster_order: int32 [32, 16], P(('grp', 'src', 'tgt')), parts along dimension 0, may hold values from 0 to 15, each once within a row
Outputs:
- potential: bfloat16 [512, 32768], P('grp', ('src', 'tgt')), parts along dimension 0
The draws below stay inside these ranges and needn't reach their ends.
There are 2 independent parts, one for each index of `grp`. The reference program is written for one: setup_inputs(seed, part) draws one part's arguments, and reference() takes and returns one part's arrays. A program takes and returns all parts, laid end to end along the dimension named above; each array names one. Nothing has to cross between parts.
Inputs may be any that keep to these rules, and one draw needn't show every extreme that they name: For every i below 8, tile_count[i] + tile_count[i + 8] == 64; slots at or beyond a device's count are unused. `cluster_order`: each row is a permutation.
All inputs are finite; a program needn't handle non-finite values.
Results may differ from the reference program's by a relative error of at most 0.007.
Values may be sent and summed in bfloat16 or wider, within the bound.
A program may use at most 128 MiB of HBM per device.

```python
import jax
import jax.numpy as jnp
from jax import lax

RHS = 128
K = 256
PC = 128
MAXT = 64
PTS = 2048
CL = 16
SHARDS = 16
PTS_ALL = 32768
LEVELS = 3
N_SRC = 8
N_TGT = 2


def draw_tile_count(key, part):
    src_total = SHARDS // N_TGT
    halfway = src_total // 2
    first_key, second_key = jax.random.split(jax.random.fold_in(key, 17))
    heavy = jax.random.randint(first_key, (halfway, N_TGT), MAXT // 2, MAXT)
    heavy = heavy.at[0, 0].set(MAXT - 1)
    light = MAXT - heavy
    flipped = jax.random.randint(second_key, (halfway, N_TGT), 0, 2)
    lower = jnp.where(flipped == 1, heavy, light)
    upper = jnp.where(flipped == 1, light, heavy)
    return jnp.concatenate([lower, upper], axis=0).reshape(SHARDS).astype(jnp.int32)


def set_ends(drawn, rng, low, top_value):
    dims = drawn.shape
    spot = [jax.random.randint(jax.random.fold_in(rng, axis), (), 0, dims[axis]) for axis in range(len(dims))]
    drawn = drawn.at[tuple(spot)].set(low)
    longest = dims.index(max(dims))
    spot[longest] = (spot[longest] + 1) % dims[longest]
    return drawn.at[tuple(spot)].set(top_value)


def level_of(key, shape, cuts, least, largest):
    factor_of, own = 1.0, jax.random.fold_in(key, 6)
    for axis_at, shards_of in cuts:
        heights = jnp.exp(jax.random.uniform(jax.random.fold_in(own, axis_at), (shards_of,), jnp.float32, least / len(cuts), largest / len(cuts)))
        factor_of = factor_of * jnp.repeat(heights, shape[axis_at] // shards_of).reshape([-1 if axis == axis_at else 1 for axis in range(len(shape))])
    return factor_of


def gaussian(key, extent, scale, limit, cuts=(), held_as=jnp.bfloat16):
    gain = level_of(key, extent, cuts, -0.22, 0.18) if cuts else 1.0
    result = jax.random.normal(key, extent, jnp.float32) * scale * gain
    return jnp.minimum(jnp.maximum(result, -limit), limit).astype(held_as)


def setup_inputs(seed: int = 0, part: int = 0) -> dict:
    key_of = jax.random.split(jax.random.key(seed), 10)
    part_splits = jax.random.split(jax.random.fold_in(key_of[9], part), 10)
    return {
        "densities": gaussian(part_splits[0], (2 * RHS, PTS_ALL), 1.0, 6.0, ((1, 16),)),
        "compress": gaussian(part_splits[1], (PTS_ALL, 2, K), (2 * N_TGT * PTS) ** -0.5, 0.0625, ((0, 16),)),
        "level_a": gaussian(part_splits[2], (LEVELS, N_SRC * K, 2, K), (4 * K) ** -0.5, 0.1875, ((1, 8), (3, 2))),
        "level_b": gaussian(part_splits[3], (LEVELS, N_SRC * K, 2, K), (4 * K) ** -0.5, 0.1875, ((1, 8), (3, 2))),
        "expand": gaussian(part_splits[4], (N_SRC * K, 2, N_TGT * PTS), (2 * K) ** -0.5, 0.25, ((0, 8), (2, 2))),
        "near_tiles": gaussian(part_splits[5], (SHARDS * MAXT, PC, 2, PC), (2 * PC) ** -0.5, 0.375, ((0, 16),)),
        "tile_pairs": set_ends(jax.random.randint(part_splits[6], (SHARDS * MAXT, 2), 0, CL), jax.random.fold_in(part_splits[6], 1), 0, CL - 1).astype(jnp.int32),
        "tile_count": draw_tile_count(jax.random.fold_in(jax.random.fold_in(key_of[9], part), 71), part),
        "cluster_order": jax.vmap(lambda own: jax.random.permutation(own, CL))(jax.random.split(part_splits[8], SHARDS)).reshape((SHARDS, CL)).astype(jnp.int32),
    }


def complex_product(operand, matrix):
    product = jnp.dot(operand, matrix, preferred_element_type=jnp.float32)
    half_rows = operand.shape[0] // 2
    half_cols = matrix.shape[1] // 2
    real_part = product[:half_rows, :half_cols] - product[half_rows:, half_cols:]
    imag_part = product[:half_rows, half_cols:] + product[half_rows:, :half_cols]
    return jnp.concatenate([real_part, imag_part], axis=0)


def near_sum(sources, tile_blocks, source_ids, target_ids, active, targets):
    half_rows = sources.shape[0] // 2
    cluster_size = tile_blocks.shape[1]
    picked = jnp.take(sources, source_ids, axis=1).astype(jnp.float32)
    product = jnp.einsum("rjp,jpq->rjq", picked, tile_blocks.astype(jnp.float32), precision=lax.Precision.HIGHEST)
    real_part = product[:half_rows, :, :cluster_size] - product[half_rows:, :, cluster_size:]
    imag_part = product[:half_rows, :, cluster_size:] + product[half_rows:, :, :cluster_size]
    joined = jnp.concatenate([real_part, imag_part], axis=0)
    chooser = ((target_ids[:, None] == jnp.arange(targets, dtype=jnp.int32)[None, :]) & active[:, None]).astype(jnp.float32)
    return jnp.einsum("rjq,jc->rcq", joined, chooser, precision=lax.Precision.HIGHEST)


def reference(densities, compress, level_a, level_b, expand, near_tiles, tile_pairs, tile_count, cluster_order):
    row_count = densities.shape[0]
    shard_dens = densities.reshape(row_count, SHARDS, PTS).transpose(1, 0, 2)
    shard_comp = compress.reshape(SHARDS, PTS, 2 * K)

    def compress_one(items):
        return complex_product(items[0], items[1])

    partial_value = lax.map(compress_one, (shard_dens, shard_comp))
    coefficients = jnp.sum(partial_value.reshape(N_SRC, N_TGT, row_count, K), axis=1).astype(jnp.bfloat16)
    full_a = level_a.reshape(LEVELS, N_SRC, K, 2 * K)
    full_b = level_b.reshape(LEVELS, N_SRC, K, 2 * K)

    def level_one(items):
        summed = complex_product(items[0], items[2]) + complex_product(items[1], items[3])
        return summed.astype(jnp.bfloat16)

    for level_index in range(LEVELS):
        partner_index = jnp.bitwise_xor(jnp.arange(N_SRC, dtype=jnp.int32), 1 << level_index)
        partner_coeff = coefficients[partner_index]
        coefficients = lax.map(level_one, (coefficients, partner_coeff, full_a[level_index], full_b[level_index]))

    shard_coeff = jnp.repeat(coefficients, N_TGT, axis=0)
    shard_expand = expand.reshape(N_SRC, K, 2, N_TGT, PTS).transpose(0, 3, 1, 2, 4).reshape(SHARDS, K, 2 * PTS)
    shard_tiles = near_tiles.reshape(SHARDS, MAXT, PC, 2 * PC)
    shard_pairs = tile_pairs.reshape(SHARDS, MAXT, 2)

    def finish_one(items):
        dens, coeff, expansion, tile_blocks, pairs, count, order = items
        far_field = complex_product(coeff, expansion).reshape(row_count, CL, PC)
        placed = jnp.zeros((row_count, CL, PC), jnp.float32).at[:, order, :].set(far_field)
        active = jnp.arange(MAXT, dtype=jnp.int32) < count
        near_field = near_sum(dens.reshape(row_count, CL, PC), tile_blocks, pairs[:, 1], pairs[:, 0], active, CL)
        return (placed + near_field).reshape(row_count, PTS).astype(jnp.bfloat16)

    results = lax.map(finish_one, (shard_dens, shard_coeff, shard_expand, shard_tiles, shard_pairs, tile_count, cluster_order))
    return results.transpose(1, 0, 2).reshape(row_count, PTS_ALL)
```

```python
import functools

import jax
import jax.numpy as jnp
from jax import lax
from jax.experimental import pallas as pl
from jax.experimental.pallas import tpu as pltpu
from jax.sharding import PartitionSpec as P

MESH = pl.DeviceIdType.MESH
CHUNKS = 2
UNROLL = 4
BF16, F32 = jnp.bfloat16, jnp.float32


def matmul(a, b):
    return jnp.dot(a, b, preferred_element_type=F32)


def spread(width, grouped):
    row = lax.broadcasted_iota(jnp.int32, (2 * width, 2 * width), 0)
    col = lax.broadcasted_iota(jnp.int32, (2 * width, 2 * width), 1)
    imag = row >= width
    point = jnp.where(imag, row - width, row)
    if grouped:
        within = point & 7
        point = (point - within) + jnp.where(within < 4, 2 * within, 2 * within - 7)
    one, zero = jnp.ones(row.shape, F32), jnp.zeros(row.shape, F32)
    signed = jnp.where(imag, -one, one)
    upper = jnp.where(jnp.where(imag, 2 * point + 1, 2 * point) == col, signed, zero)
    lower = jnp.where(jnp.where(imag, 2 * point, 2 * point + 1) == col, one, zero)
    return upper.astype(BF16), lower.astype(BF16)


def kernel(
    sizes,
    dens_h, comp_h, la_h, lb_h, exp_h, tiles_h, pairs_h, order_h, count_s,
    out_v,
    dens_v, comp_v, compd_v, lev_v, big_v, expt_v, exp_v, tiles_v, liftc_v, lifted_v, sums_v,
    part_v, part_r, coef_v, recv_v, fin_r, pairs_s, order_s,
    dens_sem, comp_sem, lev_sem, levs_sem, levr_sem, exp_sem, expt_sem, tiles_sem, part_sem, send_sem, recv_sem,
    fin_sem, table_sem,
):
    levels, clusters, width, slots, rhs, rank, n_tgt = sizes
    src, tgt = lax.axis_index("src"), lax.axis_index("tgt")
    other = 1 - tgt
    sibling = {"tgt": other}
    partners = [{"src": src ^ (1 << level)} for level in range(levels)]
    lanes = rank // width
    comp_parts = comp_sem.shape[0]
    comp_rows = comp_h.shape[0] // comp_parts
    tile_parts = tiles_sem.shape[0]
    slots_part = slots // tile_parts
    half = rhs // n_tgt
    rows = half // CHUNKS

    loads_dens = pltpu.make_async_copy(dens_h, dens_v, dens_sem)
    loads_dens.start()
    loads_comp = [
        pltpu.make_async_copy(
            comp_h.at[pl.ds(part * comp_rows, comp_rows)], comp_v.at[pl.ds(part * comp_rows, comp_rows)],
            comp_sem.at[part],
        )
        for part in range(comp_parts)
    ]
    for item in loads_comp:
        item.start()
    barrier = pltpu.get_barrier_semaphore()
    for target in [sibling] + partners:
        pl.semaphore_signal(barrier, inc=1, device_id=target, device_id_type=MESH)
    tables = ((pairs_h, pairs_s), (order_h, order_s))
    loads_tables = [pltpu.make_async_copy(*tables[i], table_sem.at[i]) for i in range(len(tables))]
    for item in loads_tables:
        item.start()
    factors = (la_h, lb_h)
    loads_lev = [pltpu.make_async_copy(factors[ab], lev_v.at[ab, tgt], lev_sem.at[ab]) for ab in range(2)]
    for item in loads_lev:
        item.start()
    loads_tiles = [
        pltpu.make_async_copy(
            tiles_h.at[pl.ds(part * slots_part, slots_part)],
            tiles_v.at[pl.ds(part * slots_part, slots_part)],
            tiles_sem.at[part],
        )
        for part in range(tile_parts)
    ]
    loads_exp = [pltpu.make_async_copy(exp_h.at[:, c], expt_v.at[c], exp_sem.at[c]) for c in range(clusters)]
    turns_exp = [
        pltpu.make_async_copy(expt_v.at[c].reshape(2 * rank, width), exp_v.at[c], expt_sem.at[c])
        for c in range(clusters)
    ]

    upper_c, lower_c = spread(width, True)
    upper, lower = spread(width, False)

    pl.semaphore_wait(barrier, 1 + levels)
    swaps_lev = [
        [
            pltpu.make_async_remote_copy(
                src_ref=factors[ab].at[level], dst_ref=lev_v.at[ab, tgt, level],
                send_sem=levs_sem.at[ab, level], recv_sem=levr_sem.at[ab, level],
                device_id=sibling, device_id_type=MESH,
            )
            for ab in range(2)
        ]
        for level in range(levels)
    ]
    for item in swaps_lev[0]:
        item.start()

    per_part = clusters // comp_parts

    def dens_half(h, c):
        cut = pl.ds(c * width, width)
        real = dens_v[pl.ds(pl.multiple_of(h * half, half), half), cut]
        imag = dens_v[pl.ds(pl.multiple_of(rhs + h * half, half), half), cut]
        return jnp.concatenate([real, imag], axis=1)

    def lift_half(h):
        for part in range(comp_parts):
            members = range(part * per_part, (part + 1) * per_part)
            stacked = jnp.concatenate([dens_half(h, c) for c in members], axis=0)
            above = matmul(stacked, upper_c).astype(BF16)
            below = matmul(stacked, lower_c).astype(BF16)
            for i, c in enumerate(members):
                cut = pl.ds(c * 2 * width, 2 * width)
                liftc_v[0:half, cut] = above[i * half : (i + 1) * half]
                liftc_v[half : 2 * half, cut] = below[i * half : (i + 1) * half]

    def split(part):
        depth = 2 * lanes * width
        even = (lax.broadcasted_iota(jnp.int32, (depth // 32, 16, width), 1) // 2) % 2 == 0
        for c in range(part * per_part, (part + 1) * per_part):
            block = comp_v[pl.ds(c * depth, depth)].reshape(depth // 32, 2, 16, width)
            first, second = block[:, 0], block[:, 1]
            left = jnp.where(even, first, pltpu.roll(second, 2, 1))
            right = jnp.where(even, pltpu.roll(first, 14, 1), second)
            compd_v[pl.ds(c * 2 * width, 2 * width), pl.ds(0, width)] = left.reshape(2 * width, width)
            compd_v[pl.ds(c * 2 * width, 2 * width), pl.ds(width, width)] = right.reshape(2 * width, width)

    def squeeze(part):
        cut = pl.ds(part * per_part * 2 * width, per_part * 2 * width)
        return matmul(liftc_v[:, cut], compd_v[cut])

    loads_dens.wait()
    lift_half(other)
    total = jnp.zeros((2 * half, rank), F32)
    for part in range(comp_parts):
        loads_comp[part].wait()
        split(part)
        total = total + squeeze(part)
    part_v[...] = total.astype(BF16)
    swap_part = pltpu.make_async_remote_copy(
        src_ref=part_v, dst_ref=part_r, send_sem=part_sem.at[0], recv_sem=part_sem.at[1],
        device_id=sibling, device_id_type=MESH,
    )
    swap_part.start()
    for item in loads_tiles:
        item.start()
    for item in loads_exp:
        item.start()
    for level in range(1, levels):
        for item in swaps_lev[level]:
            item.start()
    lift_half(tgt)
    total = jnp.zeros((2 * half, rank), F32)
    for part in range(comp_parts):
        total = total + squeeze(part)

    def prepare(level):
        for ab in range(2):
            if level == 0:
                loads_lev[ab].wait()
            swaps_lev[level][ab].wait()
            whole = jnp.concatenate([lev_v[ab, h, level] for h in range(n_tgt)], axis=1)
            for lane in range(lanes):
                block = whole[lane * 2 * width : (lane + 1) * 2 * width]
                turned = lax.dot_general(
                    gather_m, block, (((1,), (0,)), ((), ())), preferred_element_type=F32
                )
                real, imag = turned[:width].astype(BF16), turned[width:].astype(BF16)
                top, bottom = pl.ds(lane * width, width), pl.ds(rank + lane * width, width)
                big_v[ab, level, top, pl.ds(0, rank)] = real
                big_v[ab, level, top, pl.ds(rank, rank)] = imag
                big_v[ab, level, bottom, pl.ds(0, rank)] = -imag
                big_v[ab, level, bottom, pl.ds(rank, rank)] = real

    row = lax.broadcasted_iota(jnp.int32, (2 * width, 2 * width), 0)
    col = lax.broadcasted_iota(jnp.int32, (2 * width, 2 * width), 1)
    spot = jnp.where(row < width, 2 * row, 2 * (row - width) + 1)
    gather_m = jnp.where(spot == col, jnp.ones(row.shape, F32), jnp.zeros(row.shape, F32)).astype(BF16)

    def send(level, q):
        copy = pltpu.make_async_remote_copy(
            src_ref=coef_v.at[level, q], dst_ref=recv_v.at[level, q],
            send_sem=send_sem.at[level, q], recv_sem=recv_sem.at[level, q],
            device_id=partners[level], device_id_type=MESH,
        )
        copy.start()
        return copy

    for item in loads_tables:
        item.wait()
    count = count_s[0]
    last = [jnp.int32(slots) for _ in range(clusters)]
    sums_v[slots] = jnp.zeros((2 * rhs, width), F32)

    def near_step(step, last):
        last = list(last)
        base = step * UNROLL
        terms = [matmul(lifted_v[pairs_s[1, base + u]], tiles_v[base + u]) for u in range(UNROLL)]
        for u in range(UNROLL):
            slot = base + u
            target = pairs_s[0, slot]
            active = slot < count
            before = jnp.int32(slots)
            for c in range(clusters):
                hit = target == c
                before = jnp.where(hit, last[c], before)
                last[c] = jnp.where(hit & active, slot, last[c])
            sums_v[slot] = terms[u] + sums_v[before]
        return tuple(last)

    prepare(0)
    swap_part.wait()
    sends = []
    for q in range(CHUNKS):
        real = total[q * rows : (q + 1) * rows] + part_r[pl.ds(q * rows, rows)].astype(F32)
        imag = total[half + q * rows : half + (q + 1) * rows] + part_r[pl.ds(half + q * rows, rows)].astype(F32)
        coef_v[0, q] = jnp.concatenate([real, imag], axis=1).astype(BF16)
        sends.append(send(0, q))

    for c in range(clusters):
        cut = pl.ds(c * width, width)
        both = jnp.concatenate([dens_v[:rhs, cut], dens_v[rhs:, cut]], axis=1)
        lifted_v[c, :rhs] = matmul(both, upper).astype(BF16)
        lifted_v[c, rhs:] = matmul(both, lower).astype(BF16)

    current = sends
    done_sends = []
    swaps_fin = []
    for level in range(levels):
        own = matmul(
            jnp.concatenate([coef_v[level, q] for q in range(CHUNKS)], axis=0), big_v[0, level]
        )
        if level + 1 < levels:
            prepare(level + 1)
        first, final = (tile_parts * level) // levels, (tile_parts * (level + 1)) // levels
        for part in range(first, final):
            loads_tiles[part].wait()
        last = lax.fori_loop(
            first * slots_part // UNROLL, final * slots_part // UNROLL, near_step, tuple(last)
        )
        if level + 1 == levels:
            for item in turns_exp:
                item.wait()
        elif level + 2 == levels:
            for c in range(clusters):
                loads_exp[c].wait()
                turns_exp[c].start()
        following = []
        for q in range(CHUNKS):
            current[q].wait_recv()
            fresh = own[q * rows : (q + 1) * rows] + matmul(recv_v[level, q], big_v[1, level])
            coef_v[level + 1, q] = fresh.astype(BF16)
            if level + 1 < levels:
                following.append(send(level + 1, q))
            else:
                copy = pltpu.make_async_remote_copy(
                    src_ref=coef_v.at[levels, q], dst_ref=fin_r.at[q],
                    send_sem=fin_sem.at[0, q], recv_sem=fin_sem.at[1, q],
                    device_id=sibling, device_id_type=MESH,
                )
                copy.start()
                swaps_fin.append(copy)
        done_sends += current
        current = following

    origins = []
    for t in range(clusters):
        origin = jnp.int32(0)
        for c in range(clusters):
            origin = jnp.where(order_s[0, c] == t, c, origin)
        origins.append(origin)

    def finish(h, whole):
        pieces = [
            jnp.concatenate(
                [whole[:, lane * width : (lane + 1) * width], whole[:, rank + lane * width : rank + (lane + 1) * width]],
                axis=1,
            )
            for lane in range(lanes)
        ]
        operand = jnp.concatenate(
            [
                jnp.concatenate([matmul(piece, side).astype(BF16) for piece in pieces], axis=1)
                for side in (upper, lower)
            ],
            axis=0,
        )
        top = pl.ds(pl.multiple_of(h * half, half), half)
        bottom = pl.ds(pl.multiple_of(rhs + h * half, half), half)
        for t in range(0, clusters, 2):
            pair = jnp.concatenate([exp_v[origins[t]], exp_v[origins[t + 1]]], axis=1)
            far = matmul(operand, pair)
            for u in range(2):
                cut = pl.ds((t + u) * width, width)
                side = far[:, u * width : (u + 1) * width]
                out_v[top, cut] = (side[:half] + sums_v[last[t + u], top]).astype(BF16)
                out_v[bottom, cut] = (side[half:] + sums_v[last[t + u], bottom]).astype(BF16)

    finish(tgt, jnp.concatenate([coef_v[levels, q] for q in range(CHUNKS)], axis=0))
    for item in swaps_fin:
        item.wait()
    finish(other, jnp.concatenate([fin_r[q] for q in range(CHUNKS)], axis=0))
    for item in done_sends:
        item.wait_send()


def shards(
    densities, compress, level_a, level_b, expand, near_tiles, tile_pairs, tile_count, cluster_order
):
    row_count, points = densities.shape
    rhs = row_count // 2
    rank = compress.shape[2]
    levels = level_a.shape[0]
    clusters = cluster_order.shape[1]
    width = points // clusters
    slots = near_tiles.shape[0]
    n_tgt = lax.axis_size("tgt")
    sizes = (levels, clusters, width, slots, rhs, rank, n_tgt)
    lanes = rank // width
    assert lanes == 2 and n_tgt == 2
    half = rhs // n_tgt
    rows = half // CHUNKS
    comp_parts, tile_parts = 4, 16
    anywhere = pl.BlockSpec(memory_space=pl.ANY)
    dma = pltpu.SemaphoreType.DMA
    operands = (
        densities,
        compress.reshape(points, 2, lanes, width).transpose(0, 2, 1, 3).reshape(points * lanes * 2, width),
        level_a.reshape(levels, rank * 2, width),
        level_b.reshape(levels, rank * 2, width),
        expand.reshape(rank, 2, clusters, width).transpose(0, 2, 1, 3),
        near_tiles.reshape(slots, width * 2, width),
    )
    tables = (tile_pairs.T, cluster_order)
    operands = [pltpu.with_memory_space_constraint(item, pltpu.HBM) for item in operands]
    tables = [pltpu.with_memory_space_constraint(item, pltpu.HBM) for item in tables]
    return pl.pallas_call(
        functools.partial(kernel, sizes),
        out_shape=jax.ShapeDtypeStruct((row_count, points), BF16),
        in_specs=[anywhere] * 8 + [pl.BlockSpec(memory_space=pltpu.SMEM)],
        out_specs=pl.BlockSpec(memory_space=pltpu.VMEM),
        scratch_shapes=[
            pltpu.VMEM((row_count, points), BF16),
            pltpu.VMEM((points * lanes * 2, width), BF16),
            pltpu.VMEM((points * 2, rank), BF16),
            pltpu.VMEM((2, n_tgt, levels, rank * 2, width), BF16),
            pltpu.VMEM((2, levels, rank * 2, rank * 2), BF16),
            pltpu.VMEM((clusters, rank, 2, width), BF16),
            pltpu.VMEM((clusters, rank * 2, width), BF16),
            pltpu.VMEM((slots, width * 2, width), BF16),
            pltpu.VMEM((row_count // n_tgt, points * 2), BF16),
            pltpu.VMEM((clusters, row_count, 2 * width), BF16),
            pltpu.VMEM((slots + 1, row_count, width), F32),
            pltpu.VMEM((row_count // n_tgt, rank), BF16),
            pltpu.VMEM((row_count // n_tgt, rank), BF16),
            pltpu.VMEM((levels + 1, CHUNKS, rows, 2 * rank), BF16),
            pltpu.VMEM((levels, CHUNKS, rows, 2 * rank), BF16),
            pltpu.VMEM((CHUNKS, rows, 2 * rank), BF16),
            pltpu.SMEM((2, slots), jnp.int32),
            pltpu.SMEM((1, clusters), jnp.int32),
            dma,
            dma((comp_parts,)),
            dma((2,)),
            dma((2, levels)),
            dma((2, levels)),
            dma((clusters,)),
            dma((clusters,)),
            dma((tile_parts,)),
            dma((2,)),
            dma((levels, CHUNKS)),
            dma((levels, CHUNKS)),
            dma((2, CHUNKS)),
            dma((2,)),
        ],
        compiler_params=pltpu.CompilerParams(
            collective_id=0, has_side_effects=True, vmem_limit_bytes=48 << 20
        ),
    )(*operands, *tables, tile_count)


def solution(mesh):
    placed = (
        P("grp", ("src", "tgt")),
        P(("grp", "src", "tgt"), None, None),
        P("grp", "src", None, "tgt"),
        P("grp", "src", None, "tgt"),
        P(("grp", "src"), None, "tgt"),
        P(("grp", "src", "tgt"), None, None, None),
        P(("grp", "src", "tgt"), None),
        P(("grp", "src", "tgt")),
        P(("grp", "src", "tgt"), None),
    )
    return jax.shard_map(
        shards, mesh=mesh, in_specs=placed, out_specs=P("grp", ("src", "tgt")), check_vma=False
    )
```

```python
import functools

import jax
import jax.numpy as jnp
from jax import lax
from jax.experimental import pallas as pl
from jax.experimental.pallas import tpu as pltpu
from jax.sharding import PartitionSpec as P

MESH = pl.DeviceIdType.MESH
CHUNKS = 2
UNROLL = 4
BF16, F32 = jnp.bfloat16, jnp.float32


def matmul(a, b):
    return jnp.dot(a, b, preferred_element_type=F32)


def spread(width):
    row = lax.broadcasted_iota(jnp.int32, (2 * width, 2 * width), 0)
    col = lax.broadcasted_iota(jnp.int32, (2 * width, 2 * width), 1)
    imag = row >= width
    point = jnp.where(imag, row - width, row)
    one, zero = jnp.ones(row.shape, F32), jnp.zeros(row.shape, F32)
    upper = jnp.where(jnp.where(imag, 2 * point + 1, 2 * point) == col, jnp.where(imag, -one, one), zero)
    lower = jnp.where(jnp.where(imag, 2 * point, 2 * point + 1) == col, one, zero)
    return upper.astype(BF16), lower.astype(BF16)


def joined(real, imag):
    top = jnp.concatenate([real, imag], axis=1)
    bottom = jnp.concatenate([-imag, real], axis=1)
    return jnp.concatenate([top, bottom], axis=0)


def kernel(
    sizes,
    dens_h, comp_h, la_h, lb_h, exp_h, tiles_h, pairs_h, order_h, count_s,
    out_v,
    dens_v, comp_v, compd_v, lev_v, big_v, expt_v, exp_v, tiles_v, wide_v, point_v, sums_v,
    part_v, part_r, coef_v, recv_v, fin_r, pairs_s, order_s,
    dens_sem, comp_sem, lev_sem, levs_sem, levr_sem, exp_sem, expt_sem, tiles_sem, part_sem, send_sem, recv_sem,
    fin_sem, table_sem,
):
    levels, clusters, width, slots, rhs, rank, n_tgt = sizes
    src, tgt = lax.axis_index("src"), lax.axis_index("tgt")
    other = 1 - tgt
    sibling = {"tgt": other}
    partners = [{"src": src ^ (1 << level)} for level in range(levels)]
    lanes = rank // width
    comp_parts = comp_sem.shape[0]
    comp_rows = comp_h.shape[0] // comp_parts
    tile_parts = tiles_sem.shape[0]
    slots_part = slots // tile_parts
    half = rhs // n_tgt
    rows = half // CHUNKS

    loads_dens = pltpu.make_async_copy(dens_h, dens_v, dens_sem)
    loads_dens.start()
    loads_comp = [
        pltpu.make_async_copy(
            comp_h.at[pl.ds(part * comp_rows, comp_rows)], comp_v.at[pl.ds(part * comp_rows, comp_rows)],
            comp_sem.at[part],
        )
        for part in range(comp_parts)
    ]
    for item in loads_comp:
        item.start()
    barrier = pltpu.get_barrier_semaphore()
    for target in [sibling] + partners:
        pl.semaphore_signal(barrier, inc=1, device_id=target, device_id_type=MESH)
    tables = ((pairs_h, pairs_s), (order_h, order_s))
    loads_tables = [pltpu.make_async_copy(*tables[i], table_sem.at[i]) for i in range(len(tables))]
    for item in loads_tables:
        item.start()
    factors = (la_h, lb_h)
    loads_lev = [pltpu.make_async_copy(factors[ab], lev_v.at[ab, tgt], lev_sem.at[ab]) for ab in range(2)]
    for item in loads_lev:
        item.start()
    loads_tiles = [
        pltpu.make_async_copy(
            tiles_h.at[pl.ds(part * slots_part, slots_part)],
            tiles_v.at[pl.ds(part * slots_part, slots_part)],
            tiles_sem.at[part],
        )
        for part in range(tile_parts)
    ]
    loads_exp = [pltpu.make_async_copy(exp_h.at[:, c], expt_v.at[c], exp_sem) for c in range(clusters)]
    turns_exp = [
        pltpu.make_async_copy(expt_v.at[c].reshape(2 * rank, width), exp_v.at[c], expt_sem)
        for c in range(clusters)
    ]
    all_exp = pltpu.make_async_copy(expt_v, expt_v, exp_sem)
    all_turns = pltpu.make_async_copy(exp_v, exp_v, expt_sem)

    swaps_lev = [
        [
            pltpu.make_async_remote_copy(
                src_ref=factors[ab].at[level], dst_ref=lev_v.at[ab, tgt, level],
                send_sem=levs_sem.at[ab, level], recv_sem=levr_sem.at[ab, level],
                device_id=sibling, device_id_type=MESH,
            )
            for ab in range(2)
        ]
        for level in range(levels)
    ]

    per_part = clusters // comp_parts

    def parts(buffer, stride, offset):
        return wide_v[buffer, pl.ds(offset, width, stride=stride), :].astype(BF16)

    def split(c):
        depth = 2 * lanes * width
        wide_v[c % UNROLL] = comp_v[pl.ds(c * depth, depth)].astype(F32)
        for lane in range(lanes):
            for ri in range(2):
                compd_v[c, :, pl.ds(ri * rank + lane * width, width)] = parts(c % UNROLL, 2 * lanes, 2 * lane + ri)

    def squeeze(part, h):
        members = range(part * per_part, (part + 1) * per_part)
        cut = pl.ds(pl.multiple_of(h * half, half), half)
        left = jnp.concatenate([point_v[c, cut] for c in members], axis=1)
        right = jnp.concatenate([joined(compd_v[c, :, :rank], compd_v[c, :, rank:]) for c in members], axis=0)
        return matmul(left, right)

    loads_dens.wait()
    for c in range(clusters):
        cut = pl.ds(c * width, width)
        point_v[c, :, :width] = dens_v[:rhs, cut]
        point_v[c, :, width:] = dens_v[rhs:, cut]
    total = jnp.zeros((half, 2 * rank), F32)
    for part in range(comp_parts):
        loads_comp[part].wait()
        for c in range(part * per_part, (part + 1) * per_part):
            split(c)
        total = total + squeeze(part, other)
    part_v[...] = total.astype(BF16)
    swap_part = pltpu.make_async_remote_copy(
        src_ref=part_v, dst_ref=part_r, send_sem=part_sem.at[0], recv_sem=part_sem.at[1],
        device_id=sibling, device_id_type=MESH,
    )
    pl.semaphore_wait(barrier, 1 + levels)
    swap_part.start()
    for level in range(levels):
        for item in swaps_lev[level]:
            item.start()
    for item in loads_tiles:
        item.start()
    for item in loads_exp:
        item.start()
    total = jnp.zeros((half, 2 * rank), F32)
    for part in range(comp_parts):
        total = total + squeeze(part, tgt)

    def prepare(level):
        for ab in range(2):
            if level == 0:
                loads_lev[ab].wait()
            swaps_lev[level][ab].wait()
            for h in range(n_tgt):
                cells = [[None] * 2 for _ in range(lanes)]
                wide_v[2 * ab + h] = lev_v[ab, h, level].astype(F32)
                for block in range(lanes):
                    for ri in range(2):
                        cells[block][ri] = parts(2 * ab + h, 2, block * 2 * width + ri)
                for block in range(lanes):
                    real, imag = cells[block]
                    top, bottom = pl.ds(block * width, width), pl.ds(rank + block * width, width)
                    left, right = pl.ds(h * width, width), pl.ds(rank + h * width, width)
                    big_v[ab, level, top, left] = real
                    big_v[ab, level, top, right] = imag
                    big_v[ab, level, bottom, left] = -imag
                    big_v[ab, level, bottom, right] = real

    def send(level, q):
        copy = pltpu.make_async_remote_copy(
            src_ref=coef_v.at[level, q], dst_ref=recv_v.at[level, q],
            send_sem=send_sem.at[level, q], recv_sem=recv_sem.at[level, q],
            device_id=partners[level], device_id_type=MESH,
        )
        copy.start()
        return copy

    for item in loads_tables:
        item.wait()
    count = count_s[0]
    last = [jnp.int32(slots) for _ in range(clusters)]
    sums_v[slots] = jnp.zeros((rhs, 2 * width), F32)

    def near_step(step, last):
        last = list(last)
        base = step * UNROLL
        terms = []
        for u in range(UNROLL):
            wide_v[u, pl.ds(0, 2 * width), :] = tiles_v[base + u].astype(F32)
            terms.append(matmul(point_v[pairs_s[1, base + u]], joined(parts(u, 2, 0), parts(u, 2, 1))))
        for u in range(UNROLL):
            slot = base + u
            target = pairs_s[0, slot]
            active = slot < count
            before = jnp.int32(slots)
            for c in range(clusters):
                hit = target == c
                before = jnp.where(hit, last[c], before)
                last[c] = jnp.where(hit & active, slot, last[c])
            sums_v[slot] = terms[u] + sums_v[before]
        return tuple(last)

    prepare(0)
    swap_part.wait()
    sends = []
    for q in range(CHUNKS):
        cut = pl.ds(q * rows, rows)
        coef_v[0, q] = (total[q * rows : (q + 1) * rows] + part_r[cut].astype(F32)).astype(BF16)
        sends.append(send(0, q))

    upper, lower = spread(width)
    current = sends
    done_sends = []
    swaps_fin = []
    for level in range(levels):
        own = matmul(
            jnp.concatenate([coef_v[level, q] for q in range(CHUNKS)], axis=0), big_v[0, level]
        )
        if level + 1 < levels:
            prepare(level + 1)
        first, final = (tile_parts * level) // levels, (tile_parts * (level + 1)) // levels
        for part in range(first, final):
            loads_tiles[part].wait()
        last = lax.fori_loop(
            first * slots_part // UNROLL, final * slots_part // UNROLL, near_step, tuple(last)
        )
        if level + 1 == levels:
            all_turns.wait()
        elif level + 2 == levels:
            all_exp.wait()
            for item in turns_exp:
                item.start()
        following = []
        for q in range(CHUNKS):
            current[q].wait_recv()
            fresh = own[q * rows : (q + 1) * rows] + matmul(recv_v[level, q], big_v[1, level])
            coef_v[level + 1, q] = fresh.astype(BF16)
            if level + 1 < levels:
                following.append(send(level + 1, q))
            else:
                copy = pltpu.make_async_remote_copy(
                    src_ref=coef_v.at[levels, q], dst_ref=fin_r.at[q],
                    send_sem=fin_sem.at[0, q], recv_sem=fin_sem.at[1, q],
                    device_id=sibling, device_id_type=MESH,
                )
                copy.start()
                swaps_fin.append(copy)
        done_sends += current
        current = following

    origins = []
    for t in range(clusters):
        origin = jnp.int32(0)
        for c in range(clusters):
            origin = jnp.where(order_s[0, c] == t, c, origin)
        origins.append(origin)

    def finish(h, whole):
        pieces = [
            jnp.concatenate(
                [whole[:, lane * width : (lane + 1) * width], whole[:, rank + lane * width : rank + (lane + 1) * width]],
                axis=1,
            )
            for lane in range(lanes)
        ]
        operand = jnp.concatenate(
            [
                jnp.concatenate([matmul(piece, side).astype(BF16) for piece in pieces], axis=1)
                for side in (upper, lower)
            ],
            axis=0,
        )
        top = pl.ds(pl.multiple_of(h * half, half), half)
        bottom = pl.ds(pl.multiple_of(rhs + h * half, half), half)
        for t in range(0, clusters, 2):
            pair = jnp.concatenate([exp_v[origins[t]], exp_v[origins[t + 1]]], axis=1)
            far = matmul(operand, pair)
            for u in range(2):
                cut = pl.ds((t + u) * width, width)
                side = far[:, u * width : (u + 1) * width]
                out_v[top, cut] = (side[:half] + sums_v[last[t + u], top, :width]).astype(BF16)
                out_v[bottom, cut] = (side[half:] + sums_v[last[t + u], top, width:]).astype(BF16)

    finish(tgt, jnp.concatenate([coef_v[levels, q] for q in range(CHUNKS)], axis=0))
    for item in done_sends:
        item.wait_send()
    for item in swaps_fin:
        item.wait()
    finish(other, jnp.concatenate([fin_r[q] for q in range(CHUNKS)], axis=0))


def shards(
    densities, compress, level_a, level_b, expand, near_tiles, tile_pairs, tile_count, cluster_order
):
    row_count, points = densities.shape
    rhs = row_count // 2
    rank = compress.shape[2]
    levels = level_a.shape[0]
    clusters = cluster_order.shape[1]
    width = points // clusters
    slots = near_tiles.shape[0]
    n_tgt = lax.axis_size("tgt")
    sizes = (levels, clusters, width, slots, rhs, rank, n_tgt)
    lanes = rank // width
    assert lanes == 2 and n_tgt == 2 and UNROLL >= 2 * n_tgt
    half = rhs // n_tgt
    rows = half // CHUNKS
    comp_parts, tile_parts = 4, 8
    anywhere = pl.BlockSpec(memory_space=pl.ANY)
    dma = pltpu.SemaphoreType.DMA
    operands = (
        densities,
        compress.reshape(points, 2, lanes, width).transpose(0, 2, 1, 3).reshape(points * lanes * 2, width),
        level_a.reshape(levels, rank * 2, width),
        level_b.reshape(levels, rank * 2, width),
        expand.reshape(rank, 2, clusters, width).transpose(0, 2, 1, 3),
        near_tiles.reshape(slots, width * 2, width),
    )
    tables = (tile_pairs.T, cluster_order)
    operands = [pltpu.with_memory_space_constraint(item, pltpu.HBM) for item in operands]
    tables = [pltpu.with_memory_space_constraint(item, pltpu.HBM) for item in tables]
    return pl.pallas_call(
        functools.partial(kernel, sizes),
        out_shape=jax.ShapeDtypeStruct((row_count, points), BF16),
        in_specs=[anywhere] * 8 + [pl.BlockSpec(memory_space=pltpu.SMEM)],
        out_specs=pl.BlockSpec(memory_space=pltpu.VMEM),
        scratch_shapes=[
            pltpu.VMEM((row_count, points), BF16),
            pltpu.VMEM((points * lanes * 2, width), BF16),
            pltpu.VMEM((clusters, width, 2 * rank), BF16),
            pltpu.VMEM((2, n_tgt, levels, rank * 2, width), BF16),
            pltpu.VMEM((2, levels, rank * 2, rank * 2), BF16),
            pltpu.VMEM((clusters, rank, 2, width), BF16),
            pltpu.VMEM((clusters, rank * 2, width), BF16),
            pltpu.VMEM((slots, width * 2, width), BF16),
            pltpu.VMEM((UNROLL, width * 2 * lanes, width), F32),
            pltpu.VMEM((clusters, rhs, 2 * width), BF16),
            pltpu.VMEM((slots + 1, rhs, 2 * width), F32),
            pltpu.VMEM((half, 2 * rank), BF16),
            pltpu.VMEM((half, 2 * rank), BF16),
            pltpu.VMEM((levels + 1, CHUNKS, rows, 2 * rank), BF16),
            pltpu.VMEM((levels, CHUNKS, rows, 2 * rank), BF16),
            pltpu.VMEM((CHUNKS, rows, 2 * rank), BF16),
            pltpu.SMEM((2, slots), jnp.int32),
            pltpu.SMEM((1, clusters), jnp.int32),
            dma,
            dma((comp_parts,)),
            dma((2,)),
            dma((2, levels)),
            dma((2, levels)),
            dma,
            dma,
            dma((tile_parts,)),
            dma((2,)),
            dma((levels, CHUNKS)),
            dma((levels, CHUNKS)),
            dma((2, CHUNKS)),
            dma((2,)),
        ],
        compiler_params=pltpu.CompilerParams(
            collective_id=0, has_side_effects=True, vmem_limit_bytes=48 << 20
        ),
    )(*operands, *tables, tile_count)


def solution(mesh):
    placed = (
        P("grp", ("src", "tgt")),
        P(("grp", "src", "tgt"), None, None),
        P("grp", "src", None, "tgt"),
        P("grp", "src", None, "tgt"),
        P(("grp", "src"), None, "tgt"),
        P(("grp", "src", "tgt"), None, None, None),
        P(("grp", "src", "tgt"), None),
        P(("grp", "src", "tgt")),
        P(("grp", "src", "tgt"), None),
    )
    return jax.shard_map(
        shards, mesh=mesh, in_specs=placed, out_specs=P("grp", ("src", "tgt")), check_vma=False
    )
```

```python
import functools

import jax
import jax.numpy as jnp
from jax import lax
from jax.experimental import pallas as pl
from jax.experimental.pallas import tpu as pltpu
from jax.sharding import PartitionSpec as P

MESH = pl.DeviceIdType.MESH
CHUNKS = 4
UNROLL = 8
BF16, F32 = jnp.bfloat16, jnp.float32


def matmul(a, b):
    return jnp.dot(a, b, preferred_element_type=F32)


def spread(width):
    row = lax.broadcasted_iota(jnp.int32, (2 * width, 2 * width), 0)
    col = lax.broadcasted_iota(jnp.int32, (2 * width, 2 * width), 1)
    imag = row >= width
    point = jnp.where(imag, row - width, row)
    one, zero = jnp.ones(row.shape, F32), jnp.zeros(row.shape, F32)
    upper = jnp.where(jnp.where(imag, 2 * point + 1, 2 * point) == col, jnp.where(imag, -one, one), zero)
    lower = jnp.where(jnp.where(imag, 2 * point, 2 * point + 1) == col, one, zero)
    return upper.astype(BF16), lower.astype(BF16)


def joined(real, imag):
    top = jnp.concatenate([real, imag], axis=1)
    bottom = jnp.concatenate([-imag, real], axis=1)
    return jnp.concatenate([top, bottom], axis=0)


def kernel(
    sizes,
    dens_h, comp_h, la_h, lb_h, exp_h, tiles_h, pairs_h, order_h, count_s,
    out_v,
    dens_v, comp_v, compd_v, lev_v, big_v, expt_v, exp_v, tiles_v, wide_v, point_v, sums_v,
    part_v, part_r, coef_v, recv_v, fin_r, pairs_s, order_s,
    dens_sem, comp_sem, lev_sem, levs_sem, levr_sem, exp_sem, expt_sem, tiles_sem, part_sem, send_sem, recv_sem,
    fin_sem, table_sem,
):
    levels, clusters, width, slots, rhs, rank, n_tgt = sizes
    src, tgt = lax.axis_index("src"), lax.axis_index("tgt")
    other = 1 - tgt
    sibling = {"tgt": other}
    partners = [{"src": src ^ (1 << level)} for level in range(levels)]
    lanes = rank // width
    comp_parts = comp_sem.shape[0]
    comp_rows = comp_h.shape[0] // comp_parts
    tile_parts = tiles_sem.shape[0]
    slots_part = slots // tile_parts
    half = rhs // n_tgt
    rows = half // CHUNKS

    loads_dens = pltpu.make_async_copy(dens_h, dens_v, dens_sem)
    loads_dens.start()
    loads_comp = [
        pltpu.make_async_copy(
            comp_h.at[pl.ds(part * comp_rows, comp_rows)], comp_v.at[pl.ds(part * comp_rows, comp_rows)],
            comp_sem.at[part],
        )
        for part in range(comp_parts)
    ]
    for item in loads_comp:
        item.start()
    barrier = pltpu.get_barrier_semaphore()
    for target in [sibling] + partners:
        pl.semaphore_signal(barrier, inc=1, device_id=target, device_id_type=MESH)
    tables = ((pairs_h, pairs_s), (order_h, order_s))
    loads_tables = [pltpu.make_async_copy(*tables[i], table_sem.at[i]) for i in range(len(tables))]
    for item in loads_tables:
        item.start()
    factors = (la_h, lb_h)
    loads_lev = [pltpu.make_async_copy(factors[ab], lev_v.at[ab, tgt], lev_sem.at[ab]) for ab in range(2)]
    for item in loads_lev:
        item.start()
    loads_tiles = [
        pltpu.make_async_copy(
            tiles_h.at[pl.ds(part * slots_part, slots_part)],
            tiles_v.at[pl.ds(part * slots_part, slots_part)],
            tiles_sem.at[part],
        )
        for part in range(tile_parts)
    ]
    loads_exp = [pltpu.make_async_copy(exp_h.at[:, c], expt_v.at[c], exp_sem) for c in range(clusters)]
    turns_exp = [
        pltpu.make_async_copy(expt_v.at[c].reshape(2 * rank, width), exp_v.at[c], expt_sem)
        for c in range(clusters)
    ]
    all_exp = pltpu.make_async_copy(expt_v, expt_v, exp_sem)
    all_turns = pltpu.make_async_copy(exp_v, exp_v, expt_sem)

    swaps_lev = [
        [
            pltpu.make_async_remote_copy(
                src_ref=factors[ab].at[level], dst_ref=lev_v.at[ab, tgt, level],
                send_sem=levs_sem.at[ab, level], recv_sem=levr_sem.at[ab, level],
                device_id=sibling, device_id_type=MESH,
            )
            for ab in range(2)
        ]
        for level in range(levels)
    ]

    for item in loads_tiles:
        item.start()
    for item in loads_exp:
        item.start()
    per_part = clusters // comp_parts

    def parts(buffer, stride, offset):
        return wide_v[buffer, pl.ds(offset, width, stride=stride), :].astype(BF16)

    def split(c):
        depth = 2 * lanes * width
        wide_v[c % UNROLL] = comp_v[pl.ds(c * depth, depth)].astype(F32)
        for lane in range(lanes):
            for ri in range(2):
                compd_v[c, :, pl.ds(ri * rank + lane * width, width)] = parts(c % UNROLL, 2 * lanes, 2 * lane + ri)

    def squeeze(part, h):
        members = range(part * per_part, (part + 1) * per_part)
        cut = pl.ds(pl.multiple_of(h * half, half), half)
        below = pl.ds(pl.multiple_of(rhs + h * half, half), half)
        left = jnp.concatenate(
            [dens_v[side, pl.ds(c * width, width)] for c in members for side in (cut, below)], axis=1
        )
        right = jnp.concatenate([joined(compd_v[c, :, :rank], compd_v[c, :, rank:]) for c in members], axis=0)
        return matmul(left, right)

    loads_dens.wait()
    total = jnp.zeros((half, 2 * rank), F32)
    for part in range(comp_parts):
        loads_comp[part].wait()
        for c in range(part * per_part, (part + 1) * per_part):
            split(c)
        total = total + squeeze(part, other)
    part_v[...] = total.astype(BF16)
    swap_part = pltpu.make_async_remote_copy(
        src_ref=part_v, dst_ref=part_r, send_sem=part_sem.at[0], recv_sem=part_sem.at[1],
        device_id=sibling, device_id_type=MESH,
    )
    pl.semaphore_wait(barrier, 1 + levels)
    swap_part.start()
    for level in range(levels):
        for item in swaps_lev[level]:
            item.start()
    total = jnp.zeros((half, 2 * rank), F32)
    for part in range(comp_parts):
        total = total + squeeze(part, tgt)

    def prepare(level):
        for ab in range(2):
            if level == 0:
                loads_lev[ab].wait()
            swaps_lev[level][ab].wait()
            for h in range(n_tgt):
                cells = [[None] * 2 for _ in range(lanes)]
                wide_v[2 * ab + h] = lev_v[ab, h, level].astype(F32)
                for block in range(lanes):
                    for ri in range(2):
                        cells[block][ri] = parts(2 * ab + h, 2, block * 2 * width + ri)
                for block in range(lanes):
                    real, imag = cells[block]
                    top, bottom = pl.ds(block * width, width), pl.ds(rank + block * width, width)
                    left, right = pl.ds(h * width, width), pl.ds(rank + h * width, width)
                    big_v[ab, level, top, left] = real
                    big_v[ab, level, top, right] = imag
                    big_v[ab, level, bottom, left] = -imag
                    big_v[ab, level, bottom, right] = real

    def send(level, q):
        copy = pltpu.make_async_remote_copy(
            src_ref=coef_v.at[level, q], dst_ref=recv_v.at[level, q],
            send_sem=send_sem.at[level, q], recv_sem=recv_sem.at[level, q],
            device_id=partners[level], device_id_type=MESH,
        )
        copy.start()
        return copy

    for item in loads_tables:
        item.wait()
    count = count_s[0]
    last = [jnp.int32(slots) for _ in range(clusters)]
    sums_v[slots] = jnp.zeros((rhs, 2 * width), F32)

    def near_step(step, last):
        last = list(last)
        base = step * UNROLL
        terms = []
        for u in range(UNROLL):
            wide_v[u, pl.ds(0, 2 * width), :] = tiles_v[base + u].astype(F32)
            terms.append(matmul(point_v[pairs_s[1, base + u]], joined(parts(u, 2, 0), parts(u, 2, 1))))
        for u in range(UNROLL):
            slot = base + u
            target = pairs_s[0, slot]
            active = slot < count
            before = jnp.int32(slots)
            for c in range(clusters):
                hit = target == c
                before = jnp.where(hit, last[c], before)
                last[c] = jnp.where(hit & active, slot, last[c])
            sums_v[slot] = terms[u] + sums_v[before]
        return tuple(last)

    swap_part.wait()
    sends = []
    for q in range(CHUNKS):
        cut = pl.ds(q * rows, rows)
        coef_v[0, q] = (total[q * rows : (q + 1) * rows] + part_r[cut].astype(F32)).astype(BF16)
        sends.append(send(0, q))

    for c in range(clusters):
        cut = pl.ds(c * width, width)
        point_v[c, :, :width] = dens_v[:rhs, cut]
        point_v[c, :, width:] = dens_v[rhs:, cut]
    upper, lower = spread(width)
    current = sends
    done_sends = []
    swaps_fin = []
    for level in range(levels):
        prepare(level)
        own = matmul(
            jnp.concatenate([coef_v[level, q] for q in range(CHUNKS)], axis=0), big_v[0, level]
        )
        first, final = (tile_parts * level) // levels, (tile_parts * (level + 1)) // levels
        if level + 1 == levels:
            all_exp.wait()
            for item in turns_exp:
                item.start()
        for part in range(first, final):
            loads_tiles[part].wait()
        last = lax.fori_loop(
            first * slots_part // UNROLL, final * slots_part // UNROLL, near_step, tuple(last)
        )
        following = []
        for q in range(CHUNKS):
            current[q].wait_recv()
            fresh = own[q * rows : (q + 1) * rows] + matmul(recv_v[level, q], big_v[1, level])
            coef_v[level + 1, q] = fresh.astype(BF16)
            if level + 1 < levels:
                following.append(send(level + 1, q))
            else:
                copy = pltpu.make_async_remote_copy(
                    src_ref=coef_v.at[levels, q], dst_ref=fin_r.at[q],
                    send_sem=fin_sem.at[0, q], recv_sem=fin_sem.at[1, q],
                    device_id=sibling, device_id_type=MESH,
                )
                copy.start()
                swaps_fin.append(copy)
        done_sends += current
        current = following

    origins = []
    for t in range(clusters):
        origin = jnp.int32(0)
        for c in range(clusters):
            origin = jnp.where(order_s[0, c] == t, c, origin)
        origins.append(origin)

    def finish(h, whole):
        pieces = [
            jnp.concatenate(
                [whole[:, lane * width : (lane + 1) * width], whole[:, rank + lane * width : rank + (lane + 1) * width]],
                axis=1,
            )
            for lane in range(lanes)
        ]
        operand = jnp.concatenate(
            [
                jnp.concatenate([matmul(piece, side).astype(BF16) for piece in pieces], axis=1)
                for side in (upper, lower)
            ],
            axis=0,
        )
        top = pl.ds(pl.multiple_of(h * half, half), half)
        bottom = pl.ds(pl.multiple_of(rhs + h * half, half), half)
        for t in range(0, clusters, 2):
            pair = jnp.concatenate([exp_v[origins[t]], exp_v[origins[t + 1]]], axis=1)
            far = matmul(operand, pair)
            for u in range(2):
                cut = pl.ds((t + u) * width, width)
                side = far[:, u * width : (u + 1) * width]
                out_v[top, cut] = (side[:half] + sums_v[last[t + u], top, :width]).astype(BF16)
                out_v[bottom, cut] = (side[half:] + sums_v[last[t + u], top, width:]).astype(BF16)

    all_turns.wait()
    finish(tgt, jnp.concatenate([coef_v[levels, q] for q in range(CHUNKS)], axis=0))
    for item in done_sends:
        item.wait_send()
    for item in swaps_fin:
        item.wait()
    finish(other, jnp.concatenate([fin_r[q] for q in range(CHUNKS)], axis=0))


def shards(
    densities, compress, level_a, level_b, expand, near_tiles, tile_pairs, tile_count, cluster_order
):
    row_count, points = densities.shape
    rhs = row_count // 2
    rank = compress.shape[2]
    levels = level_a.shape[0]
    clusters = cluster_order.shape[1]
    width = points // clusters
    slots = near_tiles.shape[0]
    n_tgt = lax.axis_size("tgt")
    sizes = (levels, clusters, width, slots, rhs, rank, n_tgt)
    lanes = rank // width
    assert lanes == 2 and n_tgt == 2 and UNROLL >= 2 * n_tgt
    half = rhs // n_tgt
    rows = half // CHUNKS
    comp_parts, tile_parts = 4, 8
    anywhere = pl.BlockSpec(memory_space=pl.ANY)
    dma = pltpu.SemaphoreType.DMA
    operands = (
        densities,
        compress.reshape(points, 2, lanes, width).transpose(0, 2, 1, 3).reshape(points * lanes * 2, width),
        level_a.reshape(levels, rank * 2, width),
        level_b.reshape(levels, rank * 2, width),
        expand.reshape(rank, 2, clusters, width).transpose(0, 2, 1, 3),
        near_tiles.reshape(slots, width * 2, width),
    )
    tables = (tile_pairs.T, cluster_order)
    operands = [pltpu.with_memory_space_constraint(item, pltpu.HBM) for item in operands]
    tables = [pltpu.with_memory_space_constraint(item, pltpu.HBM) for item in tables]
    return pl.pallas_call(
        functools.partial(kernel, sizes),
        out_shape=jax.ShapeDtypeStruct((row_count, points), BF16),
        in_specs=[anywhere] * 8 + [pl.BlockSpec(memory_space=pltpu.SMEM)],
        out_specs=pl.BlockSpec(memory_space=pltpu.VMEM),
        scratch_shapes=[
            pltpu.VMEM((row_count, points), BF16),
            pltpu.VMEM((points * lanes * 2, width), BF16),
            pltpu.VMEM((clusters, width, 2 * rank), BF16),
            pltpu.VMEM((2, n_tgt, levels, rank * 2, width), BF16),
            pltpu.VMEM((2, levels, rank * 2, rank * 2), BF16),
            pltpu.VMEM((clusters, rank, 2, width), BF16),
            pltpu.VMEM((clusters, rank * 2, width), BF16),
            pltpu.VMEM((slots, width * 2, width), BF16),
            pltpu.VMEM((UNROLL, width * 2 * lanes, width), F32),
            pltpu.VMEM((clusters, rhs, 2 * width), BF16),
            pltpu.VMEM((slots + 1, rhs, 2 * width), F32),
            pltpu.VMEM((half, 2 * rank), BF16),
            pltpu.VMEM((half, 2 * rank), BF16),
            pltpu.VMEM((levels + 1, CHUNKS, rows, 2 * rank), BF16),
            pltpu.VMEM((levels, CHUNKS, rows, 2 * rank), BF16),
            pltpu.VMEM((CHUNKS, rows, 2 * rank), BF16),
            pltpu.SMEM((2, slots), jnp.int32),
            pltpu.SMEM((1, clusters), jnp.int32),
            dma,
            dma((comp_parts,)),
            dma((2,)),
            dma((2, levels)),
            dma((2, levels)),
            dma,
            dma,
            dma((tile_parts,)),
            dma((2,)),
            dma((levels, CHUNKS)),
            dma((levels, CHUNKS)),
            dma((2, CHUNKS)),
            dma((2,)),
        ],
        compiler_params=pltpu.CompilerParams(
            collective_id=0, has_side_effects=True, vmem_limit_bytes=48 << 20
        ),
    )(*operands, *tables, tile_count)


def solution(mesh):
    placed = (
        P("grp", ("src", "tgt")),
        P(("grp", "src", "tgt"), None, None),
        P("grp", "src", None, "tgt"),
        P("grp", "src", None, "tgt"),
        P(("grp", "src"), None, "tgt"),
        P(("grp", "src", "tgt"), None, None, None),
        P(("grp", "src", "tgt"), None),
        P(("grp", "src", "tgt")),
        P(("grp", "src", "tgt"), None),
    )
    return jax.shard_map(
        shards, mesh=mesh, in_specs=placed, out_specs=P("grp", ("src", "tgt")), check_vma=False
    )
```

```python
import functools

import jax
import jax.numpy as jnp
from jax import lax
from jax.experimental import pallas as pl
from jax.experimental.pallas import tpu as pltpu
from jax.sharding import PartitionSpec as P

MESH = pl.DeviceIdType.MESH
CHUNKS = 4
UNROLL = 8
BF16, F32 = jnp.bfloat16, jnp.float32


def matmul(a, b):
    return jnp.dot(a, b, preferred_element_type=F32)


def spread(width):
    row = lax.broadcasted_iota(jnp.int32, (2 * width, 2 * width), 0)
    col = lax.broadcasted_iota(jnp.int32, (2 * width, 2 * width), 1)
    imag = row >= width
    point = jnp.where(imag, row - width, row)
    one, zero = jnp.ones(row.shape, F32), jnp.zeros(row.shape, F32)
    upper = jnp.where(jnp.where(imag, 2 * point + 1, 2 * point) == col, jnp.where(imag, -one, one), zero)
    lower = jnp.where(jnp.where(imag, 2 * point, 2 * point + 1) == col, one, zero)
    return upper.astype(BF16), lower.astype(BF16)


def joined(real, imag):
    top = jnp.concatenate([real, imag], axis=1)
    bottom = jnp.concatenate([-imag, real], axis=1)
    return jnp.concatenate([top, bottom], axis=0)


def kernel(
    sizes,
    dens_h, comp_h, la_h, lb_h, exp_h, tiles_h, pairs_h, order_h, count_s,
    out_v,
    dens_v, comp_v, compd_v, lev_v, big_v, expt_v, exp_v, tiles_v, wide_v, point_v, sums_v,
    part_v, part_r, coef_v, recv_v, fin_r, pairs_s, order_s,
    dens_sem, comp_sem, lev_sem, levs_sem, levr_sem, exp_sem, expt_sem, tiles_sem, part_sem, send_sem, recv_sem,
    fin_sem, table_sem,
):
    levels, clusters, width, slots, rhs, rank, n_tgt = sizes
    src, tgt = lax.axis_index("src"), lax.axis_index("tgt")
    other = 1 - tgt
    sibling = {"tgt": other}
    partners = [{"src": src ^ (1 << level)} for level in range(levels)]
    lanes = rank // width
    comp_parts = comp_sem.shape[0]
    comp_rows = comp_h.shape[0] // comp_parts
    tile_parts = tiles_sem.shape[0]
    slots_part = slots // tile_parts
    half = rhs // n_tgt
    rows = half // CHUNKS

    loads_dens = pltpu.make_async_copy(dens_h, dens_v, dens_sem)
    loads_dens.start()
    loads_comp = [
        pltpu.make_async_copy(
            comp_h.at[pl.ds(part * comp_rows, comp_rows)], comp_v.at[pl.ds(part * comp_rows, comp_rows)],
            comp_sem.at[part],
        )
        for part in range(comp_parts)
    ]
    for item in loads_comp:
        item.start()
    barrier = pltpu.get_barrier_semaphore()
    for target in [sibling] + partners:
        pl.semaphore_signal(barrier, inc=1, device_id=target, device_id_type=MESH)
    tables = ((pairs_h, pairs_s), (order_h, order_s))
    loads_tables = [pltpu.make_async_copy(*tables[i], table_sem.at[i]) for i in range(len(tables))]
    for item in loads_tables:
        item.start()
    factors = (la_h, lb_h)
    loads_lev = [pltpu.make_async_copy(factors[ab], lev_v.at[ab, tgt], lev_sem.at[ab]) for ab in range(2)]
    loads_tiles = [
        pltpu.make_async_copy(
            tiles_h.at[pl.ds(part * slots_part, slots_part)],
            tiles_v.at[pl.ds(part * slots_part, slots_part)],
            tiles_sem.at[part],
        )
        for part in range(tile_parts)
    ]
    loads_exp = [pltpu.make_async_copy(exp_h.at[:, c], expt_v.at[c], exp_sem) for c in range(clusters)]
    turns_exp = [
        pltpu.make_async_copy(expt_v.at[c].reshape(2 * rank, width), exp_v.at[c], expt_sem)
        for c in range(clusters)
    ]
    all_exp = pltpu.make_async_copy(expt_v, expt_v, exp_sem)
    all_turns = pltpu.make_async_copy(exp_v, exp_v, expt_sem)

    swaps_lev = [
        [
            pltpu.make_async_remote_copy(
                src_ref=factors[ab].at[level], dst_ref=lev_v.at[ab, tgt, level],
                send_sem=levs_sem.at[ab, level], recv_sem=levr_sem.at[ab, level],
                device_id=sibling, device_id_type=MESH,
            )
            for ab in range(2)
        ]
        for level in range(levels)
    ]

    per_part = clusters // comp_parts

    def parts(buffer, stride, offset):
        return wide_v[buffer, pl.ds(offset, width, stride=stride), :].astype(BF16)

    def split(c):
        depth = 2 * lanes * width
        wide_v[c % UNROLL] = comp_v[pl.ds(c * depth, depth)].astype(F32)
        for lane in range(lanes):
            for ri in range(2):
                compd_v[c, :, pl.ds(ri * rank + lane * width, width)] = parts(c % UNROLL, 2 * lanes, 2 * lane + ri)

    def squeeze(part, h):
        members = range(part * per_part, (part + 1) * per_part)
        cut = pl.ds(pl.multiple_of(h * half, half), half)
        below = pl.ds(pl.multiple_of(rhs + h * half, half), half)
        left = jnp.concatenate(
            [dens_v[side, pl.ds(c * width, width)] for c in members for side in (cut, below)], axis=1
        )
        right = jnp.concatenate([joined(compd_v[c, :, :rank], compd_v[c, :, rank:]) for c in members], axis=0)
        return matmul(left, right)

    loads_dens.wait()
    total = jnp.zeros((half, 2 * rank), F32)
    for part in range(comp_parts):
        loads_comp[part].wait()
        for c in range(part * per_part, (part + 1) * per_part):
            split(c)
        total = total + squeeze(part, other)
    for item in loads_tiles:
        item.start()
    for item in loads_exp:
        item.start()
    for item in loads_lev:
        item.start()
    part_v[...] = total.astype(BF16)
    swap_part = pltpu.make_async_remote_copy(
        src_ref=part_v, dst_ref=part_r, send_sem=part_sem.at[0], recv_sem=part_sem.at[1],
        device_id=sibling, device_id_type=MESH,
    )
    pl.semaphore_wait(barrier, 1 + levels)
    swap_part.start()
    for level in range(levels):
        for item in swaps_lev[level]:
            item.start()
    total = jnp.zeros((half, 2 * rank), F32)
    for part in range(comp_parts):
        total = total + squeeze(part, tgt)

    def prepare(level):
        for ab in range(2):
            if level == 0:
                loads_lev[ab].wait()
            swaps_lev[level][ab].wait()
            for h in range(n_tgt):
                cells = [[None] * 2 for _ in range(lanes)]
                wide_v[2 * ab + h] = lev_v[ab, h, level].astype(F32)
                for block in range(lanes):
                    for ri in range(2):
                        cells[block][ri] = parts(2 * ab + h, 2, block * 2 * width + ri)
                for block in range(lanes):
                    real, imag = cells[block]
                    top, bottom = pl.ds(block * width, width), pl.ds(rank + block * width, width)
                    left, right = pl.ds(h * width, width), pl.ds(rank + h * width, width)
                    big_v[ab, level, top, left] = real
                    big_v[ab, level, top, right] = imag
                    big_v[ab, level, bottom, left] = -imag
                    big_v[ab, level, bottom, right] = real

    def send(level, q):
        copy = pltpu.make_async_remote_copy(
            src_ref=coef_v.at[level, q], dst_ref=recv_v.at[level, q],
            send_sem=send_sem.at[level, q], recv_sem=recv_sem.at[level, q],
            device_id=partners[level], device_id_type=MESH,
        )
        copy.start()
        return copy

    for item in loads_tables:
        item.wait()
    count = count_s[0]
    last = [jnp.int32(slots) for _ in range(clusters)]
    sums_v[slots] = jnp.zeros((rhs, 2 * width), F32)

    def near_step(step, last):
        last = list(last)
        base = step * UNROLL
        terms = []
        for u in range(UNROLL):
            wide_v[u, pl.ds(0, 2 * width), :] = tiles_v[base + u].astype(F32)
            terms.append(matmul(point_v[pairs_s[1, base + u]], joined(parts(u, 2, 0), parts(u, 2, 1))))
        for u in range(UNROLL):
            slot = base + u
            target = pairs_s[0, slot]
            active = slot < count
            before = jnp.int32(slots)
            for c in range(clusters):
                hit = target == c
                before = jnp.where(hit, last[c], before)
                last[c] = jnp.where(hit & active, slot, last[c])
            sums_v[slot] = terms[u] + sums_v[before]
        return tuple(last)

    swap_part.wait()
    sends = []
    for q in range(CHUNKS):
        cut = pl.ds(q * rows, rows)
        coef_v[0, q] = (total[q * rows : (q + 1) * rows] + part_r[cut].astype(F32)).astype(BF16)
        sends.append(send(0, q))

    for c in range(clusters):
        cut = pl.ds(c * width, width)
        point_v[c, :, :width] = dens_v[:rhs, cut]
        point_v[c, :, width:] = dens_v[rhs:, cut]
    upper, lower = spread(width)
    current = sends
    done_sends = []
    swaps_fin = []
    for level in range(levels):
        prepare(level)
        own = matmul(
            jnp.concatenate([coef_v[level, q] for q in range(CHUNKS)], axis=0), big_v[0, level]
        )
        first, final = (tile_parts * level) // levels, (tile_parts * (level + 1)) // levels
        if level + 1 == levels:
            all_exp.wait()
            for item in turns_exp:
                item.start()
        for part in range(first, final):
            loads_tiles[part].wait()
        last = lax.fori_loop(
            first * slots_part // UNROLL, final * slots_part // UNROLL, near_step, tuple(last)
        )
        following = []
        for q in range(CHUNKS):
            current[q].wait_recv()
            fresh = own[q * rows : (q + 1) * rows] + matmul(recv_v[level, q], big_v[1, level])
            coef_v[level + 1, q] = fresh.astype(BF16)
            if level + 1 < levels:
                following.append(send(level + 1, q))
            else:
                copy = pltpu.make_async_remote_copy(
                    src_ref=coef_v.at[levels, q], dst_ref=fin_r.at[q],
                    send_sem=fin_sem.at[0, q], recv_sem=fin_sem.at[1, q],
                    device_id=sibling, device_id_type=MESH,
                )
                copy.start()
                swaps_fin.append(copy)
        done_sends += current
        current = following

    origins = []
    for t in range(clusters):
        origin = jnp.int32(0)
        for c in range(clusters):
            origin = jnp.where(order_s[0, c] == t, c, origin)
        origins.append(origin)

    def finish(h, whole):
        pieces = [
            jnp.concatenate(
                [whole[:, lane * width : (lane + 1) * width], whole[:, rank + lane * width : rank + (lane + 1) * width]],
                axis=1,
            )
            for lane in range(lanes)
        ]
        operand = jnp.concatenate(
            [
                jnp.concatenate([matmul(piece, side).astype(BF16) for piece in pieces], axis=1)
                for side in (upper, lower)
            ],
            axis=0,
        )
        top = pl.ds(pl.multiple_of(h * half, half), half)
        bottom = pl.ds(pl.multiple_of(rhs + h * half, half), half)
        for t in range(0, clusters, 2):
            pair = jnp.concatenate([exp_v[origins[t]], exp_v[origins[t + 1]]], axis=1)
            far = matmul(operand, pair)
            for u in range(2):
                cut = pl.ds((t + u) * width, width)
                side = far[:, u * width : (u + 1) * width]
                out_v[top, cut] = (side[:half] + sums_v[last[t + u], top, :width]).astype(BF16)
                out_v[bottom, cut] = (side[half:] + sums_v[last[t + u], top, width:]).astype(BF16)

    all_turns.wait()
    finish(tgt, jnp.concatenate([coef_v[levels, q] for q in range(CHUNKS)], axis=0))
    for item in done_sends:
        item.wait_send()
    for item in swaps_fin:
        item.wait()
    finish(other, jnp.concatenate([fin_r[q] for q in range(CHUNKS)], axis=0))


def shards(
    densities, compress, level_a, level_b, expand, near_tiles, tile_pairs, tile_count, cluster_order
):
    row_count, points = densities.shape
    rhs = row_count // 2
    rank = compress.shape[2]
    levels = level_a.shape[0]
    clusters = cluster_order.shape[1]
    width = points // clusters
    slots = near_tiles.shape[0]
    n_tgt = lax.axis_size("tgt")
    sizes = (levels, clusters, width, slots, rhs, rank, n_tgt)
    lanes = rank // width
    assert lanes == 2 and n_tgt == 2 and UNROLL >= 2 * n_tgt
    half = rhs // n_tgt
    rows = half // CHUNKS
    comp_parts, tile_parts = 4, 8
    anywhere = pl.BlockSpec(memory_space=pl.ANY)
    dma = pltpu.SemaphoreType.DMA
    operands = (
        densities,
        compress.reshape(points, 2, lanes, width).transpose(0, 2, 1, 3).reshape(points * lanes * 2, width),
        level_a.reshape(levels, rank * 2, width),
        level_b.reshape(levels, rank * 2, width),
        expand.reshape(rank, 2, clusters, width).transpose(0, 2, 1, 3),
        near_tiles.reshape(slots, width * 2, width),
    )
    tables = (tile_pairs.T, cluster_order)
    operands = [pltpu.with_memory_space_constraint(item, pltpu.HBM) for item in operands]
    tables = [pltpu.with_memory_space_constraint(item, pltpu.HBM) for item in tables]
    return pl.pallas_call(
        functools.partial(kernel, sizes),
        out_shape=jax.ShapeDtypeStruct((row_count, points), BF16),
        in_specs=[anywhere] * 8 + [pl.BlockSpec(memory_space=pltpu.SMEM)],
        out_specs=pl.BlockSpec(memory_space=pltpu.VMEM),
        scratch_shapes=[
            pltpu.VMEM((row_count, points), BF16),
            pltpu.VMEM((points * lanes * 2, width), BF16),
            pltpu.VMEM((clusters, width, 2 * rank), BF16),
            pltpu.VMEM((2, n_tgt, levels, rank * 2, width), BF16),
            pltpu.VMEM((2, levels, rank * 2, rank * 2), BF16),
            pltpu.VMEM((clusters, rank, 2, width), BF16),
            pltpu.VMEM((clusters, rank * 2, width), BF16),
            pltpu.VMEM((slots, width * 2, width), BF16),
            pltpu.VMEM((UNROLL, width * 2 * lanes, width), F32),
            pltpu.VMEM((clusters, rhs, 2 * width), BF16),
            pltpu.VMEM((slots + 1, rhs, 2 * width), F32),
            pltpu.VMEM((half, 2 * rank), BF16),
            pltpu.VMEM((half, 2 * rank), BF16),
            pltpu.VMEM((levels + 1, CHUNKS, rows, 2 * rank), BF16),
            pltpu.VMEM((levels, CHUNKS, rows, 2 * rank), BF16),
            pltpu.VMEM((CHUNKS, rows, 2 * rank), BF16),
            pltpu.SMEM((2, slots), jnp.int32),
            pltpu.SMEM((1, clusters), jnp.int32),
            dma,
            dma((comp_parts,)),
            dma((2,)),
            dma((2, levels)),
            dma((2, levels)),
            dma,
            dma,
            dma((tile_parts,)),
            dma((2,)),
            dma((levels, CHUNKS)),
            dma((levels, CHUNKS)),
            dma((2, CHUNKS)),
            dma((2,)),
        ],
        compiler_params=pltpu.CompilerParams(
            collective_id=0, has_side_effects=True, vmem_limit_bytes=48 << 20
        ),
    )(*operands, *tables, tile_count)


def solution(mesh):
    placed = (
        P("grp", ("src", "tgt")),
        P(("grp", "src", "tgt"), None, None),
        P("grp", "src", None, "tgt"),
        P("grp", "src", None, "tgt"),
        P(("grp", "src"), None, "tgt"),
        P(("grp", "src", "tgt"), None, None, None),
        P(("grp", "src", "tgt"), None),
        P(("grp", "src", "tgt")),
        P(("grp", "src", "tgt"), None),
    )
    return jax.shard_map(
        shards, mesh=mesh, in_specs=placed, out_specs=P("grp", ("src", "tgt")), check_vma=False
    )
```

```python
import functools

import jax
import jax.numpy as jnp
from jax import lax
from jax.experimental import pallas as pl
from jax.experimental.pallas import tpu as pltpu
from jax.sharding import PartitionSpec as P

MESH = pl.DeviceIdType.MESH
CHUNKS = 4
UNROLL = 8
BF16, F32 = jnp.bfloat16, jnp.float32


def matmul(a, b):
    return jnp.dot(a, b, preferred_element_type=F32)


def spread(width):
    row = lax.broadcasted_iota(jnp.int32, (2 * width, 2 * width), 0)
    col = lax.broadcasted_iota(jnp.int32, (2 * width, 2 * width), 1)
    imag = row >= width
    point = jnp.where(imag, row - width, row)
    one, zero = jnp.ones(row.shape, F32), jnp.zeros(row.shape, F32)
    upper = jnp.where(jnp.where(imag, 2 * point + 1, 2 * point) == col, jnp.where(imag, -one, one), zero)
    lower = jnp.where(jnp.where(imag, 2 * point, 2 * point + 1) == col, one, zero)
    return upper.astype(BF16), lower.astype(BF16)


def joined(real, imag):
    top = jnp.concatenate([real, imag], axis=1)
    bottom = jnp.concatenate([-imag, real], axis=1)
    return jnp.concatenate([top, bottom], axis=0)


def kernel(
    sizes,
    dens_h, comp_h, la_h, lb_h, exp_h, tiles_h, pairs_h, order_h, count_s,
    out_v,
    dens_v, comp_v, compd_v, lev_v, big_v, expt_v, exp_v, tiles_v, wide_v, point_v, sums_v,
    part_v, part_r, coef_v, recv_v, fin_r, pairs_s, order_s,
    dens_sem, comp_sem, lev_sem, levs_sem, levr_sem, exp_sem, expt_sem, tiles_sem, part_sem, send_sem, recv_sem,
    fin_sem, table_sem,
):
    levels, clusters, width, slots, rhs, rank, n_tgt = sizes
    src, tgt = lax.axis_index("src"), lax.axis_index("tgt")
    other = 1 - tgt
    sibling = {"tgt": other}
    partners = [{"src": src ^ (1 << level)} for level in range(levels)]
    lanes = rank // width
    comp_parts = comp_sem.shape[0]
    comp_rows = comp_h.shape[0] // comp_parts
    tile_parts = tiles_sem.shape[0]
    slots_part = slots // tile_parts
    half = rhs // n_tgt
    rows = half // CHUNKS

    loads_dens = pltpu.make_async_copy(dens_h, dens_v, dens_sem)
    loads_dens.start()
    loads_comp = [
        pltpu.make_async_copy(
            comp_h.at[pl.ds(part * comp_rows, comp_rows)], comp_v.at[pl.ds(part * comp_rows, comp_rows)],
            comp_sem.at[part],
        )
        for part in range(comp_parts)
    ]
    for item in loads_comp:
        item.start()
    barrier = pltpu.get_barrier_semaphore()
    for target in [sibling] + partners:
        pl.semaphore_signal(barrier, inc=1, device_id=target, device_id_type=MESH)
    tables = ((pairs_h, pairs_s), (order_h, order_s))
    loads_tables = [pltpu.make_async_copy(*tables[i], table_sem.at[i]) for i in range(len(tables))]
    for item in loads_tables:
        item.start()
    factors = (la_h, lb_h)
    loads_lev = [pltpu.make_async_copy(factors[ab], lev_v.at[ab, tgt], lev_sem.at[ab]) for ab in range(2)]
    loads_tiles = [
        pltpu.make_async_copy(
            tiles_h.at[pl.ds(part * slots_part, slots_part)],
            tiles_v.at[pl.ds(part * slots_part, slots_part)],
            tiles_sem.at[part],
        )
        for part in range(tile_parts)
    ]
    loads_exp = [pltpu.make_async_copy(exp_h.at[:, c], expt_v.at[c], exp_sem) for c in range(clusters)]
    turns_exp = [
        pltpu.make_async_copy(expt_v.at[c].reshape(2 * rank, width), exp_v.at[c], expt_sem)
        for c in range(clusters)
    ]
    all_exp = pltpu.make_async_copy(expt_v, expt_v, exp_sem)
    all_turns = pltpu.make_async_copy(exp_v, exp_v, expt_sem)

    swaps_lev = [
        [
            pltpu.make_async_remote_copy(
                src_ref=factors[ab].at[level], dst_ref=lev_v.at[ab, tgt, level],
                send_sem=levs_sem.at[ab, level], recv_sem=levr_sem.at[ab, level],
                device_id=sibling, device_id_type=MESH,
            )
            for ab in range(2)
        ]
        for level in range(levels)
    ]

    per_part = clusters // comp_parts

    def parts(buffer, stride, offset):
        return wide_v[buffer, pl.ds(offset, width, stride=stride), :].astype(BF16)

    def split(c):
        depth = 2 * lanes * width
        wide_v[c % UNROLL] = comp_v[pl.ds(c * depth, depth)].astype(F32)
        for lane in range(lanes):
            for ri in range(2):
                compd_v[c, :, pl.ds(ri * rank + lane * width, width)] = parts(c % UNROLL, 2 * lanes, 2 * lane + ri)

    def squeeze(part, h):
        members = range(part * per_part, (part + 1) * per_part)
        cut = pl.ds(pl.multiple_of(h * half, half), half)
        below = pl.ds(pl.multiple_of(rhs + h * half, half), half)
        left = jnp.concatenate(
            [dens_v[side, pl.ds(c * width, width)] for c in members for side in (cut, below)], axis=1
        )
        right = jnp.concatenate([joined(compd_v[c, :, :rank], compd_v[c, :, rank:]) for c in members], axis=0)
        return matmul(left, right)

    loads_dens.wait()
    total = jnp.zeros((half, 2 * rank), F32)
    for part in range(comp_parts):
        loads_comp[part].wait()
        for c in range(part * per_part, (part + 1) * per_part):
            split(c)
        total = total + squeeze(part, other)
    for item in loads_tiles:
        item.start()
    for item in loads_exp:
        item.start()
    for item in loads_lev:
        item.start()
    part_v[...] = total.astype(BF16)
    swap_part = pltpu.make_async_remote_copy(
        src_ref=part_v, dst_ref=part_r, send_sem=part_sem.at[0], recv_sem=part_sem.at[1],
        device_id=sibling, device_id_type=MESH,
    )
    pl.semaphore_wait(barrier, 1 + levels)
    swap_part.start()
    for level in range(levels):
        for item in swaps_lev[level]:
            item.start()
    total = jnp.zeros((half, 2 * rank), F32)
    for part in range(comp_parts):
        total = total + squeeze(part, tgt)

    def prepare(level):
        for ab in range(2):
            if level == 0:
                loads_lev[ab].wait()
            swaps_lev[level][ab].wait()
            for h in range(n_tgt):
                cells = [[None] * 2 for _ in range(lanes)]
                wide_v[2 * ab + h] = lev_v[ab, h, level].astype(F32)
                for block in range(lanes):
                    for ri in range(2):
                        cells[block][ri] = parts(2 * ab + h, 2, block * 2 * width + ri)
                for block in range(lanes):
                    real, imag = cells[block]
                    top, bottom = pl.ds(block * width, width), pl.ds(rank + block * width, width)
                    left, right = pl.ds(h * width, width), pl.ds(rank + h * width, width)
                    big_v[ab, level, top, left] = real
                    big_v[ab, level, top, right] = imag
                    big_v[ab, level, bottom, left] = -imag
                    big_v[ab, level, bottom, right] = real

    def send(level, q):
        copy = pltpu.make_async_remote_copy(
            src_ref=coef_v.at[level, q], dst_ref=recv_v.at[level, q],
            send_sem=send_sem, recv_sem=recv_sem.at[level, q],
            device_id=partners[level], device_id_type=MESH,
        )
        copy.start()
        return copy

    for item in loads_tables:
        item.wait()
    count = count_s[0]
    last = [jnp.int32(slots) for _ in range(clusters)]
    sums_v[slots] = jnp.zeros((rhs, 2 * width), F32)

    def near_step(step, last):
        last = list(last)
        base = step * UNROLL
        terms = []
        for u in range(UNROLL):
            wide_v[u, pl.ds(0, 2 * width), :] = tiles_v[base + u].astype(F32)
            terms.append(matmul(point_v[pairs_s[1, base + u]], joined(parts(u, 2, 0), parts(u, 2, 1))))
        for u in range(UNROLL):
            slot = base + u
            target = pairs_s[0, slot]
            active = slot < count
            before = jnp.int32(slots)
            for c in range(clusters):
                hit = target == c
                before = jnp.where(hit, last[c], before)
                last[c] = jnp.where(hit & active, slot, last[c])
            sums_v[slot] = terms[u] + sums_v[before]
        return tuple(last)

    swap_part.wait()
    sends = []
    for q in range(CHUNKS):
        cut = pl.ds(q * rows, rows)
        coef_v[0, q] = (total[q * rows : (q + 1) * rows] + part_r[cut].astype(F32)).astype(BF16)
        sends.append(send(0, q))

    for c in range(clusters):
        cut = pl.ds(c * width, width)
        point_v[c, :, :width] = dens_v[:rhs, cut]
        point_v[c, :, width:] = dens_v[rhs:, cut]
    upper, lower = spread(width)
    current = sends
    for level in range(levels):
        prepare(level)
        own = matmul(
            jnp.concatenate([coef_v[level, q] for q in range(CHUNKS)], axis=0), big_v[0, level]
        )
        first, final = (tile_parts * level) // levels, (tile_parts * (level + 1)) // levels
        if level + 1 == levels:
            all_exp.wait()
            for item in turns_exp:
                item.start()
        for part in range(first, final):
            loads_tiles[part].wait()
        last = lax.fori_loop(
            first * slots_part // UNROLL, final * slots_part // UNROLL, near_step, tuple(last)
        )
        following = []
        for q in range(CHUNKS):
            current[q].wait_recv()
            fresh = own[q * rows : (q + 1) * rows] + matmul(recv_v[level, q], big_v[1, level])
            coef_v[level + 1, q] = fresh.astype(BF16)
            if level + 1 < levels:
                following.append(send(level + 1, q))
            else:
                copy = pltpu.make_async_remote_copy(
                    src_ref=coef_v.at[levels, q], dst_ref=fin_r.at[q],
                    send_sem=fin_sem.at[0], recv_sem=fin_sem.at[1],
                    device_id=sibling, device_id_type=MESH,
                )
                copy.start()
        current = following

    origins = []
    for t in range(clusters):
        origin = jnp.int32(0)
        for c in range(clusters):
            origin = jnp.where(order_s[0, c] == t, c, origin)
        origins.append(origin)

    def finish(h, whole):
        pieces = [
            jnp.concatenate(
                [whole[:, lane * width : (lane + 1) * width], whole[:, rank + lane * width : rank + (lane + 1) * width]],
                axis=1,
            )
            for lane in range(lanes)
        ]
        operand = jnp.concatenate(
            [
                jnp.concatenate([matmul(piece, side).astype(BF16) for piece in pieces], axis=1)
                for side in (upper, lower)
            ],
            axis=0,
        )
        top = pl.ds(pl.multiple_of(h * half, half), half)
        bottom = pl.ds(pl.multiple_of(rhs + h * half, half), half)
        for t in range(0, clusters, 2):
            pair = jnp.concatenate([exp_v[origins[t]], exp_v[origins[t + 1]]], axis=1)
            far = matmul(operand, pair)
            for u in range(2):
                cut = pl.ds((t + u) * width, width)
                side = far[:, u * width : (u + 1) * width]
                out_v[top, cut] = (side[:half] + sums_v[last[t + u], top, :width]).astype(BF16)
                out_v[bottom, cut] = (side[half:] + sums_v[last[t + u], top, width:]).astype(BF16)

    all_turns.wait()
    finish(tgt, jnp.concatenate([coef_v[levels, q] for q in range(CHUNKS)], axis=0))
    pltpu.make_async_copy(recv_v, recv_v, send_sem).wait()
    for i in range(2):
        pltpu.make_async_copy(fin_r, fin_r, fin_sem.at[i]).wait()
    finish(other, jnp.concatenate([fin_r[q] for q in range(CHUNKS)], axis=0))


def shards(
    densities, compress, level_a, level_b, expand, near_tiles, tile_pairs, tile_count, cluster_order
):
    row_count, points = densities.shape
    rhs = row_count // 2
    rank = compress.shape[2]
    levels = level_a.shape[0]
    clusters = cluster_order.shape[1]
    width = points // clusters
    slots = near_tiles.shape[0]
    n_tgt = lax.axis_size("tgt")
    sizes = (levels, clusters, width, slots, rhs, rank, n_tgt)
    lanes = rank // width
    assert lanes == 2 and n_tgt == 2 and UNROLL >= 2 * n_tgt
    half = rhs // n_tgt
    rows = half // CHUNKS
    comp_parts, tile_parts = 4, 8
    anywhere = pl.BlockSpec(memory_space=pl.ANY)
    dma = pltpu.SemaphoreType.DMA
    operands = (
        densities,
        compress.reshape(points, 2, lanes, width).transpose(0, 2, 1, 3).reshape(points * lanes * 2, width),
        level_a.reshape(levels, rank * 2, width),
        level_b.reshape(levels, rank * 2, width),
        expand.reshape(rank, 2, clusters, width).transpose(0, 2, 1, 3),
        near_tiles.reshape(slots, width * 2, width),
    )
    tables = (tile_pairs.T, cluster_order)
    operands = [pltpu.with_memory_space_constraint(item, pltpu.HBM) for item in operands]
    tables = [pltpu.with_memory_space_constraint(item, pltpu.HBM) for item in tables]
    return pl.pallas_call(
        functools.partial(kernel, sizes),
        out_shape=jax.ShapeDtypeStruct((row_count, points), BF16),
        in_specs=[anywhere] * 8 + [pl.BlockSpec(memory_space=pltpu.SMEM)],
        out_specs=pl.BlockSpec(memory_space=pltpu.VMEM),
        scratch_shapes=[
            pltpu.VMEM((row_count, points), BF16),
            pltpu.VMEM((points * lanes * 2, width), BF16),
            pltpu.VMEM((clusters, width, 2 * rank), BF16),
            pltpu.VMEM((2, n_tgt, levels, rank * 2, width), BF16),
            pltpu.VMEM((2, levels, rank * 2, rank * 2), BF16),
            pltpu.VMEM((clusters, rank, 2, width), BF16),
            pltpu.VMEM((clusters, rank * 2, width), BF16),
            pltpu.VMEM((slots, width * 2, width), BF16),
            pltpu.VMEM((UNROLL, width * 2 * lanes, width), F32),
            pltpu.VMEM((clusters, rhs, 2 * width), BF16),
            pltpu.VMEM((slots + 1, rhs, 2 * width), F32),
            pltpu.VMEM((half, 2 * rank), BF16),
            pltpu.VMEM((half, 2 * rank), BF16),
            pltpu.VMEM((levels + 1, CHUNKS, rows, 2 * rank), BF16),
            pltpu.VMEM((levels, CHUNKS, rows, 2 * rank), BF16),
            pltpu.VMEM((CHUNKS, rows, 2 * rank), BF16),
            pltpu.SMEM((2, slots), jnp.int32),
            pltpu.SMEM((1, clusters), jnp.int32),
            dma,
            dma((comp_parts,)),
            dma((2,)),
            dma((2, levels)),
            dma((2, levels)),
            dma,
            dma,
            dma((tile_parts,)),
            dma((2,)),
            dma,
            dma((levels, CHUNKS)),
            dma((2,)),
            dma((2,)),
        ],
        compiler_params=pltpu.CompilerParams(
            collective_id=0, has_side_effects=True, vmem_limit_bytes=48 << 20
        ),
    )(*operands, *tables, tile_count)


def solution(mesh):
    placed = (
        P("grp", ("src", "tgt")),
        P(("grp", "src", "tgt"), None, None),
        P("grp", "src", None, "tgt"),
        P("grp", "src", None, "tgt"),
        P(("grp", "src"), None, "tgt"),
        P(("grp", "src", "tgt"), None, None, None),
        P(("grp", "src", "tgt"), None),
        P(("grp", "src", "tgt")),
        P(("grp", "src", "tgt"), None),
    )
    return jax.shard_map(
        shards, mesh=mesh, in_specs=placed, out_specs=P("grp", ("src", "tgt")), check_vma=False
    )
```
